32 devices in a mesh: table: 16 (over z, y, x), dp: 2 (over core).
Axes of the slice: x: 2, y: 2, z: 4, core: 2. Of those that a mesh axis runs over, the one named last changes fastest.
Arguments:
- tables: bfloat16 [4, 65536, 128], P(None, 'table'), may hold values from -6 to 6
- owner_ids: int32 [32, 4, 256, 1], P(('table', 'dp')), may hold values from 0 to 15; in each aligned block of 256 rows (0 to 255, 256 to 511, ..., all dimensions but the last counted through in order) at most 32 rows name the same one
- row_ids: int32 [32, 4, 256], P(('table', 'dp')), may hold values from 0 to 4095
- session_of: int32 [32, 256], P(('table', 'dp')), may hold values from 0 to 1, never falling along the last dimension, each value on 1 to 200 neighbouring positions
- relevance: float32 [32, 256], P(('table', 'dp')), may hold values from 0.1 to 10
- logit_bias: float32 [32, 256], P(('table', 'dp')), may hold values from -400 to 400
- w_hidden: float32 [512, 512], replicated, may hold values from -0.25 to 0.25
- bias_hidden: float32 [512], replicated, may hold values from -3 to 3
- w_score: float32 [512], replicated, may hold values from -0.9 to 0.9
Outputs:
- emb_step: float32 [4, 65536, 128], P(None, ('table', 'dp'))
- step_hidden: float32 [512, 512], replicated
- step_bias: float32 [512], replicated
- step_score: float32 [512], replicated
- loss: float32 [], replicated
The draws below stay inside these ranges and needn't reach their ends.
Inputs may be any that keep to these rules, and one draw needn't show every extreme that they name: `owner_ids`: among one device's impressions, for one table, at most 32 name the same owner. `session_of`: session numbers never fall along a device's impressions; each of a device's 2 sessions has 1 to 200 impressions.
All inputs are finite; a program needn't handle non-finite values.
Results may differ from the reference program's by a relative error of at most 0.001.
The reference program's roundings to bfloat16 on the way (of `inputs`, `hidden_bf`, `pre_grad_bf` and `input_grad`) count: a program that leaves them out, or rounds other values in their place, can miss the bound.
Values may be sent and summed in bfloat16 or wider, within the bound.
A program may use at most 64 MiB of HBM per device.

```python
import math
import jax
import jax.numpy as jnp
import numpy as np
from jax import lax

EMB = 128
ROWS_DEV = 4096
TABLES = 4
HID = 512
SLOTS = 200
SESS_DEV = 2
IMP_DEV = 256
CAP = 32
FEAT = 512
ROWS = 65536
SESSIONS = 64
N_TABLE = 16
DEVICES = 32


def draw_logit_bias(key, part):
    key_base = jax.random.fold_in(jax.random.fold_in(key, 71), 0)
    return jnp.clip(jax.random.normal(key_base, (DEVICES, IMP_DEV), jnp.float32), -6.0, 6.0)


def with_ends(drawn, key, low, largest):
    dims = drawn.shape
    spot = [jax.random.randint(jax.random.fold_in(key, axis), (), 0, dims[axis]) for axis in range(len(dims))]
    drawn = drawn.at[tuple(spot)].set(low)
    longest = dims.index(max(dims))
    spot[longest] = (spot[longest] + 1) % dims[longest]
    return drawn.at[tuple(spot)].set(largest)


def block_levels(stream_key, dims, cuts, low, high):
    factor_of, own = 1.0, jax.random.fold_in(stream_key, 6)
    for axis_at, shards_of in cuts:
        steps = jnp.exp(jax.random.uniform(jax.random.fold_in(own, axis_at), (shards_of,), jnp.float32, low / len(cuts), high / len(cuts)))
        factor_of = factor_of * jnp.repeat(steps, dims[axis_at] // shards_of).reshape([-1 if axis == axis_at else 1 for axis in range(len(dims))])
    return factor_of


def rank_bounds(number_of, lean):
    weights = [(1 << 20) // math.isqrt(grade ** lean) + 1 for grade in range(1, number_of + 1)]
    deviation = 1 + sum(weights) // (1 << 30)
    return np.cumsum(np.array([max(1, weight // deviation) for weight in weights]))


def skewed_ids(rng, shape, count, lean):
    table = rank_bounds(count, lean)
    pick = jax.random.randint(jax.random.fold_in(rng, 1), shape, 0, int(table[count - 1]))
    rank = jnp.searchsorted(jnp.asarray(table, jnp.int32), pick, side="right")
    return jax.random.permutation(jax.random.fold_in(rng, 2), count)[rank].astype(jnp.int32)


def split_up(number_of, total, bound, skew):
    portions = [(1 << 20) // math.isqrt(rank ** skew) + 1 for rank in range(2, number_of + 1)]
    surplus, counts = total - bound - (number_of - 1), [1] * (number_of - 1)
    while surplus > 0:
        movable = [i for i in range(number_of - 1) if counts[i] < bound]
        pool, left = sum([portions[i] for i in movable]), surplus
        for i in movable:
            addition = min(bound - counts[i], max(1, left * portions[i] // pool), surplus)
            counts[i] = counts[i] + addition
            surplus = surplus - addition
    return np.array([bound] + counts)


def ragged(own_key, number_of, total, most, slope):
    if number_of == 2:
        one = jax.random.randint(own_key, (), max(1, total - most), min(most, total - 1) + 1)
        return jnp.stack([one, total - one])
    sizes = jnp.asarray(split_up(number_of, total, most, slope), jnp.int32)
    couples = (number_of - 1) // 2
    donor, receiver = sizes[1:1 + 2 * couples:2], sizes[2:2 + 2 * couples:2]
    room = jnp.minimum(donor - 1, most - receiver)
    moved = jax.random.randint(jax.random.fold_in(own_key, 1), (couples,), 0, 1 << 20) % (room + 1)
    sizes = sizes.at[1:1 + 2 * couples:2].set(donor - moved).at[2:2 + 2 * couples:2].set(receiver + moved)
    return sizes[jax.random.permutation(jax.random.fold_in(own_key, 2), number_of)]


def assign_block(own_key, own, number, rows, count, top, limit, slope):
    ranking = jax.random.permutation(own_key, count)
    heavy_load, usual = portions_of(count, rows * top, limit, slope, True), portions_of(count, rows * top, limit, slope, False)
    places = jnp.arange(count)

    def named(lengths, rotation):
        used = int((lengths > 0).sum())
        fixed = max(1, used // 4)
        moved = fixed + (places - fixed + rotation * (used - fixed)) % max(1, count - fixed)
        return jnp.zeros((count,), jnp.int32).at[ranking[jnp.where(places < fixed, places, moved)]].set(jnp.asarray(lengths, jnp.int32))

    lengths = jnp.where(number % 4 == 0, named(heavy_load, number // 4), named(usual, number - number // 4 - 1))
    mixed = jax.random.permutation(jax.random.fold_in(own, 3), count)
    giver, sink = mixed[0:count // 2 * 2:2], mixed[1:count // 2 * 2:2]
    room = jnp.minimum(lengths[giver] - 1, limit - lengths[sink]) // 2
    room = jnp.where((giver == ranking[0]) | (sink == ranking[0]) | (lengths[sink] == 0), 0, jnp.maximum(room, 0))
    moved = jax.random.randint(jax.random.fold_in(own, 4), (count // 2,), 0, 1 << 20) % (room + 1)
    lengths = lengths.at[giver].add(-moved).at[sink].add(moved)
    labels = jnp.searchsorted(jnp.cumsum(lengths), jnp.arange(rows * top), side="right").astype(jnp.int32)
    grid = labels.reshape(top, rows).T
    grid = grid[jax.random.permutation(jax.random.fold_in(own, 1), rows)]
    rotation = jax.random.randint(jax.random.fold_in(own, 2), (rows, 1), 0, top)
    return jnp.take_along_axis(grid, (jnp.arange(top)[None, :] + rotation) % top, axis=1)


def portions_of(amount, total, reach, slope, full):
    loads = [(1 << 20) // math.isqrt(rank ** slope) + 1 for rank in range(1, amount + 1)]
    largest = reach if full else min(reach, max(-(-total // amount), total * loads[0] // sum(loads)))
    least = 1 if total - largest >= amount - 1 else 0
    counts, surplus = [largest] + [least] * (amount - 1), total - largest - least * (amount - 1)
    while surplus > 0:
        candidates = [i for i in range(1, amount) if counts[i] < largest] or [i for i in range(1, amount) if counts[i] < reach]
        pool, left = sum([loads[i] for i in candidates]), surplus
        for i in candidates:
            more = min(reach - counts[i], max(1, left * loads[i] // pool), surplus)
            counts[i] = counts[i] + more
            surplus = surplus - more
    return np.array(counts)


def normal_values(rng, extent, spread, most, cuts=(), kind=jnp.bfloat16):
    array = jax.random.normal(rng, extent, jnp.float32) * spread
    if len(cuts) > 0:
        array = block_levels(rng, extent, cuts, -0.22, 0.18) * array
    return jnp.clip(array, min=-most, max=most).astype(kind)


def setup_inputs(seed: int = 0) -> dict:
    streams_of = jax.random.split(jax.random.key(seed), 10)
    tables = normal_values(streams_of[0], (TABLES, ROWS, EMB), 1.0, 6.0, ((1, 16),))
    owner_ids_keys = jax.random.split(jax.random.fold_in(streams_of[1], 1), DEVICES * TABLES * IMP_DEV // IMP_DEV)
    owner_ids_turns = jax.random.permutation(jax.random.fold_in(streams_of[1], 3), DEVICES * TABLES * IMP_DEV // IMP_DEV)
    owner_ids = jax.vmap(lambda own, number: assign_block(jax.random.fold_in(streams_of[1], 2), own, number, IMP_DEV, N_TABLE, 1, CAP, 1))(owner_ids_keys, owner_ids_turns).reshape((DEVICES, TABLES, IMP_DEV, 1))
    row_ids = with_ends(skewed_ids(streams_of[2], (DEVICES, TABLES, IMP_DEV), ROWS_DEV, 2), jax.random.fold_in(streams_of[2], 3), 0, ROWS_DEV - 1).astype(jnp.int32)
    session_of = jax.vmap(lambda own: jnp.searchsorted(jnp.cumsum(ragged(own, SESS_DEV, IMP_DEV, SLOTS, 1)), jnp.arange(IMP_DEV), side="right"))(jax.random.split(streams_of[3], DEVICES)).reshape((DEVICES, IMP_DEV)).astype(jnp.int32)
    relevance = jnp.clip(jnp.exp(math.log(10.0) - 4.6051702 * jax.random.uniform(streams_of[4], (DEVICES, IMP_DEV), jnp.float32) ** block_levels(streams_of[4], (DEVICES, IMP_DEV), ((0, 32),), -0.2, 0.2)), 0.1, 10.0)
    logit_bias = draw_logit_bias(jax.random.fold_in(streams_of[9], 71), 0)
    w_hidden = normal_values(streams_of[6], (FEAT, HID), FEAT ** -0.5, 0.25, (), jnp.float32)
    bias_hidden = normal_values(streams_of[7], (HID,), 0.5, 3.0, (), jnp.float32)
    w_score = normal_values(streams_of[8], (HID,), 0.15, 0.9, (), jnp.float32)
    return {"tables": tables, "owner_ids": owner_ids, "row_ids": row_ids, "session_of": session_of, "relevance": relevance, "logit_bias": logit_bias, "w_hidden": w_hidden, "bias_hidden": bias_hidden, "w_score": w_score}


def silu_slope(pre_val):
    logistic = jax.nn.sigmoid(pre_val)
    return logistic * (1.0 + pre_val * (1.0 - logistic))

def session_terms(scores, session_ids, relevance, sessions):
    member = session_ids[None, :] == jnp.arange(sessions, dtype=jnp.int32)[:, None]
    highest = lax.optimization_barrier(jnp.max(jnp.where(member, scores[None, :], -jnp.inf), axis=1))
    highest_each = lax.optimization_barrier(jnp.sum(jnp.where(member, highest[:, None], 0.0), axis=0))
    shifted = scores - highest_each
    exponent = jnp.exp(shifted)
    totals = lax.optimization_barrier(jnp.sum(jnp.where(member, exponent[None, :], 0.0), axis=1))
    weights = lax.optimization_barrier(jnp.sum(jnp.where(member, relevance[None, :], 0.0), axis=1))
    total_each = lax.optimization_barrier(jnp.sum(jnp.where(member, totals[:, None], 0.0), axis=0))
    weight_each = lax.optimization_barrier(jnp.sum(jnp.where(member, weights[:, None], 0.0), axis=0))
    probability = exponent / total_each
    target = relevance / weight_each
    loss_sum = jnp.sum(jnp.log(totals)) - jnp.sum(target * shifted)
    return (loss_sum, probability - target)

def reference(tables, owner_ids, row_ids, session_of, relevance, logit_bias, w_hidden, bias_hidden, w_score):
    hidden_bf = w_hidden.astype(jnp.bfloat16)
    global_rows = owner_ids[:, :, :, 0] * ROWS_DEV + row_ids
    table_index = jnp.arange(TABLES, dtype=jnp.int32)

    def block_step(carry, block):
        weight_acc, bias_acc, score_acc, loss_acc = carry
        rows_here, session_ids, relevant, bias_row = block
        fetched = tables[table_index[None, :], rows_here.T]
        inputs = fetched.reshape(IMP_DEV, TABLES * EMB)
        pre_act = jnp.dot(inputs, hidden_bf, preferred_element_type=jnp.float32) + bias_hidden
        hidden = jax.nn.silu(pre_act)
        scores = jnp.dot(hidden, w_score, precision=lax.Precision.HIGHEST) + bias_row
        loss_sum, score_grad = session_terms(scores, session_ids, relevant, SESS_DEV)
        pre_grad = score_grad[:, None] * w_score[None, :] * silu_slope(pre_act)
        pre_grad_bf = pre_grad.astype(jnp.bfloat16)
        weight_grad = lax.dot_general(inputs, pre_grad_bf, (((0,), (0,)), ((), ())), preferred_element_type=jnp.float32)
        bias_grad = lax.optimization_barrier(jnp.sum(pre_grad, axis=0))
        score_weight_grad = jnp.dot(score_grad, hidden, precision=lax.Precision.HIGHEST)
        input_grad = jnp.dot(pre_grad_bf, hidden_bf.T, preferred_element_type=jnp.float32).astype(jnp.bfloat16)
        carry = (weight_acc + weight_grad, bias_acc + bias_grad, score_acc + score_weight_grad, loss_acc + loss_sum)
        return (carry, input_grad.reshape(IMP_DEV, TABLES, EMB))
    init = (jnp.zeros((FEAT, HID), jnp.float32), jnp.zeros((HID,), jnp.float32), jnp.zeros((HID,), jnp.float32), jnp.zeros((), jnp.float32))
    totals, grads = lax.scan(block_step, init, (global_rows, session_of, relevance, logit_bias))
    weight_tot, bias_tot, score_tot, loss_tot = totals
    row_grad = jnp.zeros((TABLES, ROWS, EMB), jnp.float32)
    row_grad = row_grad.at[table_index[None, None, :], jnp.transpose(global_rows, (0, 2, 1))].add(grads.astype(jnp.float32))
    emb_step = row_grad / (jnp.sqrt(lax.optimization_barrier(jnp.mean(row_grad * row_grad, axis=2, keepdims=True))) + 1e-06)
    param_count = FEAT * HID + 2 * HID
    mean_sq = (jnp.sum(weight_tot * weight_tot) + jnp.sum(bias_tot * bias_tot) + jnp.sum(score_tot * score_tot)) / param_count
    factor = 1.0 / jnp.sqrt(mean_sq + 1e-06)
    loss = loss_tot / SESSIONS
    return (emb_step, weight_tot * factor, bias_tot * factor, score_tot * factor, loss)
```

```python
import jax
import jax.numpy as jnp
from jax import lax
from jax.experimental import pallas as pl
from jax.experimental.pallas import tpu as pltpu
import functools
from jax.sharding import PartitionSpec as P

SESS_DEV = 2


def silu_slope(pre_val):
    logistic = jax.nn.sigmoid(pre_val)
    return logistic * (1.0 + pre_val * (1.0 - logistic))


def session_terms(scores, session_ids, relevance, sessions):
    member = session_ids[None, :] == jnp.arange(sessions, dtype=jnp.int32)[:, None]
    highest = jnp.max(jnp.where(member, scores[None, :], -jnp.inf), axis=1)
    highest_each = jnp.sum(jnp.where(member, highest[:, None], 0.0), axis=0)
    shifted = scores - highest_each
    exponent = jnp.exp(shifted)
    totals = jnp.sum(jnp.where(member, exponent[None, :], 0.0), axis=1)
    weights = jnp.sum(jnp.where(member, relevance[None, :], 0.0), axis=1)
    total_each = jnp.sum(jnp.where(member, totals[:, None], 0.0), axis=0)
    weight_each = jnp.sum(jnp.where(member, weights[:, None], 0.0), axis=0)
    probability = exponent / total_each
    target = relevance / weight_each
    loss_sum = jnp.sum(jnp.log(totals)) - jnp.sum(target * shifted)
    return (loss_sum, probability - target)


def selector(indices, count):
    return (indices[:, None] == jnp.arange(count, dtype=jnp.int32)[None, :]).astype(jnp.bfloat16)


def pick_rows(indices, source):
    return jnp.dot(
        selector(indices, source.shape[0]), source, preferred_element_type=jnp.float32
    ).astype(jnp.bfloat16)


def place_rows(indices, values, count):
    return lax.dot_general(
        selector(indices, count),
        values,
        (((0,), (0,)), ((), ())),
        preferred_element_type=jnp.float32,
    )


def on_device(
    tables, owner_ids, row_ids, session_of, relevance, logit_bias, w_hidden, bias_hidden, w_score
):
    owners = lax.axis_size("table")
    devices = owners * lax.axis_size("dp")
    table_count, shard_rows, emb_width = tables.shape
    owner_now = owner_ids[0, :, :, 0]
    rows_now = row_ids[0]
    imp_count = owner_now.shape[1]
    capacity = 2 * imp_count // owners
    slot_total = owners * capacity
    one_hot = (owner_now[:, :, None] == jnp.arange(owners, dtype=jnp.int32)).astype(jnp.float32)
    places = jnp.arange(imp_count, dtype=jnp.int32)
    lower_tri = (places[:, None] >= places[None, :]).astype(jnp.float32)
    running = jnp.einsum("ij,tjo->tio", lower_tri, one_hot, precision=lax.Precision.HIGHEST)
    rank_in = (jnp.sum(running * one_hot, axis=2) - 1.0).astype(jnp.int32)
    slot_of = owner_now * capacity + rank_in
    slot_hot = (slot_of[:, :, None] == jnp.arange(slot_total, dtype=jnp.int32)).astype(jnp.int32)
    wanted = jnp.sum(slot_hot * rows_now[:, :, None], axis=1) + shard_rows * (
        1 - jnp.sum(slot_hot, axis=1)
    )
    requested = lax.all_to_all(
        wanted.reshape(table_count, owners, capacity),
        "table",
        split_axis=1,
        concat_axis=1,
        tiled=True,
    )
    served = lax.map(
        lambda pair: pick_rows(pair[0], pair[1]),
        (requested.reshape(table_count, slot_total), tables),
    )
    served = served.reshape(table_count, owners, capacity, emb_width)
    hidden_bf = w_hidden.astype(jnp.bfloat16)
    returned = lax.all_to_all(served, "table", split_axis=1, concat_axis=1, tiled=True).reshape(
        table_count, slot_total, emb_width
    )
    gathered = lax.map(lambda pair: pick_rows(pair[0], pair[1]), (slot_of, returned))
    inputs = jnp.transpose(gathered, (1, 0, 2)).reshape(imp_count, table_count * emb_width)
    pre_act = jnp.dot(inputs, hidden_bf, preferred_element_type=jnp.float32)
    pre_act = pre_act + bias_hidden
    hidden = jax.nn.silu(pre_act)
    scores = jnp.dot(hidden, w_score, precision=lax.Precision.HIGHEST) + logit_bias[0]
    loss_sum, score_grad = session_terms(scores, session_of[0], relevance[0], SESS_DEV)
    pre_grad = score_grad[:, None] * w_score[None, :] * silu_slope(pre_act)
    pre_grad_bf = pre_grad.astype(jnp.bfloat16)
    weight_grad = lax.dot_general(
        inputs, pre_grad_bf, (((0,), (0,)), ((), ())), preferred_element_type=jnp.float32
    )
    bias_grad = jnp.sum(pre_grad, axis=0)
    score_weight_grad = jnp.dot(score_grad, hidden, precision=lax.Precision.HIGHEST)
    input_grad = jnp.dot(pre_grad_bf, hidden_bf.T, preferred_element_type=jnp.float32).astype(
        jnp.bfloat16
    )
    input_grad = jnp.transpose(input_grad.reshape(imp_count, table_count, emb_width), (1, 0, 2))
    outgoing = lax.map(
        lambda pair: place_rows(pair[0], pair[1], slot_total).astype(jnp.bfloat16),
        (slot_of, input_grad),
    )
    if capacity % 16 == 0 and w_hidden.shape[0] == w_hidden.shape[1]:
        return finish_kernel(
            outgoing.reshape(table_count, owners, capacity, emb_width),
            requested.reshape(table_count, slot_total),
            weight_grad,
            bias_grad,
            score_weight_grad,
            loss_sum,
            shard_rows,
        )
    incoming = lax.all_to_all(
        outgoing.reshape(table_count, owners, capacity, emb_width),
        "table",
        split_axis=1,
        concat_axis=1,
        tiled=True,
    )
    summed = lax.map(
        lambda pair: place_rows(pair[0], pair[1], shard_rows),
        (
            requested.reshape(table_count, slot_total),
            incoming.reshape(table_count, slot_total, emb_width),
        ),
    )
    own_rows = lax.psum_scatter(summed, "dp", scatter_dimension=1, tiled=True)
    emb_step = own_rows / (jnp.sqrt(jnp.mean(own_rows * own_rows, axis=2, keepdims=True)) + 1e-06)
    param_count = w_hidden.size + bias_hidden.size + w_score.size
    weight_tot, bias_tot, score_tot, loss_tot = lax.psum(
        (weight_grad, bias_grad, score_weight_grad, loss_sum), ("table", "dp")
    )
    mean_sq = (
        jnp.sum(weight_tot * weight_tot)
        + jnp.sum(bias_tot * bias_tot)
        + jnp.sum(score_tot * score_tot)
    ) / param_count
    factor = 1.0 / jnp.sqrt(mean_sq + 1e-06)
    step_hidden = weight_tot * factor
    loss = loss_tot / (SESS_DEV * devices)
    return (emb_step, step_hidden, bias_tot * factor, score_tot * factor, loss)


MESH = pl.DeviceIdType.MESH


def finish_body(
    sizes, out_ref, ids_ref, dense_ref, emb_ref, step_ref, small_ref,
    grads, swapped, ids_other, emb_rows, from_other, from_plane, from_column, sum_pair, sum_plane,
    total, grad_send, grad_recv, own_sem, swap_send, swap_recv, ids_sems, pair_sems, plane_send,
    plane_recv, column_send, column_recv, emb_sem,
):
    tables, owners, capacity, width, half_rows, inner, outer, hid, sessions = sizes
    slots = owners * capacity
    me = lax.axis_index("table")
    core = lax.axis_index("dp")
    low, high = lax.rem(me, inner), me // inner
    other = (me, 1 - core)

    barrier = pltpu.get_barrier_semaphore()

    def greet(step, carry):
        pl.semaphore_signal(
            barrier, inc=1, device_id=(lax.rem(me + step, owners), core), device_id_type=MESH
        )
        return carry

    pl.semaphore_signal(barrier, inc=1, device_id=other, device_id_type=MESH)
    lax.fori_loop(1, owners, greet, 0)
    pl.semaphore_wait(barrier, owners)

    def remote(src, dst, send, recv, to):
        return pltpu.make_async_remote_copy(
            src_ref=src, dst_ref=dst, send_sem=send, recv_sem=recv, device_id=to,
            device_id_type=MESH,
        )

    pair_up = remote(dense_ref.at[1 - core], from_other, pair_sems.at[0], pair_sems.at[1], other)
    pair_up.start()
    ids_copy = remote(ids_ref, ids_other, ids_sems.at[0], ids_sems.at[1], other)
    ids_copy.start()

    def own_copy(table):
        return pltpu.make_async_copy(
            out_ref.at[table, me], grads.at[table, me], own_sem.at[table]
        )

    def send_grads(table):
        own_copy(table).start()

        def send_one(step, carry):
            owner = lax.rem(me + step, owners)
            remote(
                out_ref.at[table, owner], grads.at[table, me], grad_send.at[table],
                grad_recv.at[table], (owner, core),
            ).start()
            return carry

        lax.fori_loop(1, owners, send_one, 0)

    def all_grads(table):
        return remote(
            out_ref.at[table, pl.ds(0, owners - 1)], grads.at[table, pl.ds(0, owners - 1)],
            grad_send.at[table], grad_recv.at[table], other,
        )

    def swap(table):
        return remote(
            grads.at[table], swapped.at[table], swap_send.at[table], swap_recv.at[table], other
        )

    def arrive(table):
        own_copy(table).wait()
        all_grads(table).wait()
        swap(table).start()

    block = 256

    def emb_copy(table):
        return pltpu.make_async_copy(emb_rows.at[table], emb_ref.at[table], emb_sem.at[table])

    def place(table):
        swap(table).wait()
        ids_mine = ids_ref[pl.ds(table, 1), :]
        ids_theirs = ids_other[pl.ds(table, 1), :]
        rows_mine = grads[table].reshape(slots, width)
        rows_theirs = swapped[table].reshape(slots, width)

        def place_block(step, carry):
            at = lax.broadcasted_iota(jnp.int32, (block, slots), 0) + (
                core * half_rows + step * block
            )
            hot_mine = jnp.where(at == ids_mine, 1.0, 0.0).astype(jnp.bfloat16)
            hot_theirs = jnp.where(at == ids_theirs, 1.0, 0.0).astype(jnp.bfloat16)
            summed = jnp.dot(hot_mine, rows_mine, preferred_element_type=jnp.float32)
            summed = summed + jnp.dot(hot_theirs, rows_theirs, preferred_element_type=jnp.float32)
            mean = jnp.sum(summed * summed, axis=1, keepdims=True) / width
            emb_rows[table, pl.ds(pl.multiple_of(step * block, block), block), :] = summed / (
                jnp.sqrt(mean) + 1e-06
            )
            return carry

        lax.fori_loop(0, half_rows // block, place_block, 0)
        emb_copy(table).start()

    def plane_copies(phase, src_of, dst_of):
        return [
            remote(
                src_of(lax.rem(low + step, inner)), dst_of(step - 1), plane_send.at[phase, step - 1],
                plane_recv.at[phase, step - 1], (high * inner + lax.rem(low + step, inner), core),
            )
            for step in range(1, inner)
        ]

    def column_copies(phase, src_of, dst_of):
        return [
            remote(
                src_of(lax.rem(high + step, outer)), dst_of(step - 1), column_send.at[phase, step - 1],
                column_recv.at[phase, step - 1], (lax.rem(high + step, outer) * inner + low, core),
            )
            for step in range(1, outer)
        ]

    def run(copies):
        for copy in copies:
            copy.start()

    def finish(copies):
        for copy in copies:
            copy.wait()

    send_grads(0)
    pair_up.wait()
    sum_pair[...] = dense_ref[core] + from_other[...]
    plane_sum = plane_copies(0, lambda to: sum_pair.at[to], lambda slot: from_plane.at[slot])
    run(plane_sum)
    for table in range(1, tables):
        send_grads(table)
    ids_copy.wait()
    finish(plane_sum)
    part = sum_pair[low]
    for slot in range(inner - 1):
        part = part + from_plane[slot]
    sum_plane[...] = part
    column_sum = column_copies(0, lambda to: sum_plane.at[to], lambda slot: from_column.at[slot])
    run(column_sum)
    arrive(0)
    finish(column_sum)
    part = sum_plane[high]
    for slot in range(outer - 1):
        part = part + from_column[slot]
    total[core, low, high] = part
    column_share = column_copies(
        1, lambda to: total.at[core, low, high], lambda slot: total.at[core, low, high]
    )
    run(column_share)
    place(0)
    for table in range(1, tables):
        if table == 1:
            finish(column_share)
            plane_share = plane_copies(
                1, lambda to: total.at[core, low], lambda slot: total.at[core, low]
            )
            run(plane_share)
        arrive(table)
        if table == tables - 1:
            finish(plane_share)
            pair_down = remote(
                total.at[core], total.at[core], pair_sems.at[2], pair_sems.at[3], other
            )
            pair_down.start()
        place(table)
    pair_down.wait()
    every = total[...].reshape(2 * owners * dense_ref.shape[3], dense_ref.shape[4])
    weights, extra = every[:, :hid], every[:, hid:]
    counted = lax.broadcasted_iota(jnp.int32, extra.shape, 1) < 2
    counts = jnp.where(counted, extra, 0.0)
    squares = jnp.sum(weights * weights, keepdims=True) + jnp.sum(counts * counts, keepdims=True)
    factor = 1.0 / jnp.sqrt(squares / (hid * hid + 2 * hid) + 1e-06)
    step_ref[...] = weights * factor
    scaled = jnp.where(counted, extra * factor, extra / sessions)
    small_ref[...] = scaled.T
    for table in range(tables):
        emb_copy(table).wait()


def finish_kernel(outgoing, requested, weight_grad, bias_grad, score_grad, loss_sum, shard_rows):
    tables, owners, capacity, width = outgoing.shape
    hid = weight_grad.shape[0]
    half_rows = shard_rows // 2
    inner = 1
    while inner * inner < owners:
        inner *= 2
    outer = owners // inner
    rows = hid // (2 * owners)
    lane = jnp.arange(128, dtype=jnp.int32)[None, :]
    extra = jnp.where(
        lane == 0,
        bias_grad[:, None],
        jnp.where(
            lane == 1,
            score_grad[:, None],
            jnp.where(
                (lane == 2) & (jnp.arange(hid, dtype=jnp.int32)[:, None] == 0), loss_sum, 0.0
            ),
        ),
    )
    dense = jnp.concatenate([weight_grad, extra], axis=1)
    wide = dense.shape[1]
    dense = dense.reshape(2, inner, outer, rows, wide)
    sizes = (
        tables, owners, capacity, width, half_rows, inner, outer, hid,
        SESS_DEV * owners * 2,
    )
    f32, bf16 = jnp.float32, jnp.bfloat16
    dma = pltpu.SemaphoreType.DMA
    vmem = pl.BlockSpec(memory_space=pltpu.VMEM)
    emb_step, step_hidden, small = pl.pallas_call(
        functools.partial(finish_body, sizes),
        out_shape=(
            jax.ShapeDtypeStruct((tables, half_rows, width), f32),
            jax.ShapeDtypeStruct((hid, hid), f32),
            jax.ShapeDtypeStruct((128, hid), f32),
        ),
        in_specs=[vmem] * 3,
        out_specs=(pl.BlockSpec(memory_space=pl.ANY), vmem, vmem),
        scratch_shapes=[
            pltpu.VMEM((tables, owners, capacity, width), bf16),
            pltpu.VMEM((tables, owners, capacity, width), bf16),
            pltpu.VMEM(requested.shape, jnp.int32),
            pltpu.VMEM((tables, half_rows, width), f32),
            pltpu.VMEM((inner, outer, rows, wide), f32),
            pltpu.VMEM((inner - 1, outer, rows, wide), f32),
            pltpu.VMEM((outer - 1, rows, wide), f32),
            pltpu.VMEM((inner, outer, rows, wide), f32),
            pltpu.VMEM((outer, rows, wide), f32),
            pltpu.VMEM((2, inner, outer, rows, wide), f32),
            dma((tables,)), dma((tables,)), dma((tables,)), dma((tables,)), dma((tables,)),
            dma((2,)), dma((4,)),
            dma((2, inner - 1)), dma((2, inner - 1)), dma((2, outer - 1)), dma((2, outer - 1)),
            dma((tables,)),
        ],
        compiler_params=pltpu.CompilerParams(collective_id=1, has_side_effects=True),
    )(outgoing, requested, dense)
    return (emb_step, step_hidden, small[0], small[1], small[2, 0])


def solution(mesh):
    in_specs = (
        P(None, "table", None),
        P(("table", "dp"), None, None, None),
        P(("table", "dp"), None, None),
        P(("table", "dp"), None),
        P(("table", "dp"), None),
        P(("table", "dp"), None),
        P(),
        P(),
        P(),
    )
    out_specs = (P(None, ("table", "dp"), None), P(), P(), P(), P())
    return jax.shard_map(
        on_device, mesh=mesh, in_specs=in_specs, out_specs=out_specs, check_vma=False
    )
```

```python
import jax
import jax.numpy as jnp
from jax import lax
from jax.experimental import pallas as pl
from jax.experimental.pallas import tpu as pltpu
import functools
from jax.sharding import PartitionSpec as P

SESS_DEV = 2


def silu_slope(pre_val):
    logistic = jax.nn.sigmoid(pre_val)
    return logistic * (1.0 + pre_val * (1.0 - logistic))


def session_terms(scores, session_ids, relevance, sessions):
    member = session_ids[None, :] == jnp.arange(sessions, dtype=jnp.int32)[:, None]
    highest = jnp.max(jnp.where(member, scores[None, :], -jnp.inf), axis=1)
    highest_each = jnp.sum(jnp.where(member, highest[:, None], 0.0), axis=0)
    shifted = scores - highest_each
    exponent = jnp.exp(shifted)
    totals = jnp.sum(jnp.where(member, exponent[None, :], 0.0), axis=1)
    weights = jnp.sum(jnp.where(member, relevance[None, :], 0.0), axis=1)
    total_each = jnp.sum(jnp.where(member, totals[:, None], 0.0), axis=0)
    weight_each = jnp.sum(jnp.where(member, weights[:, None], 0.0), axis=0)
    probability = exponent / total_each
    target = relevance / weight_each
    loss_sum = jnp.sum(jnp.log(totals)) - jnp.sum(target * shifted)
    return (loss_sum, probability - target)


def selector(indices, count):
    return (indices[:, None] == jnp.arange(count, dtype=jnp.int32)[None, :]).astype(jnp.bfloat16)


def pick_rows(indices, source):
    return jnp.dot(
        selector(indices, source.shape[0]), source, preferred_element_type=jnp.float32
    ).astype(jnp.bfloat16)


def place_rows(indices, values, count):
    return lax.dot_general(
        selector(indices, count),
        values,
        (((0,), (0,)), ((), ())),
        preferred_element_type=jnp.float32,
    )


def on_device(
    tables, owner_ids, row_ids, session_of, relevance, logit_bias, w_hidden, bias_hidden, w_score
):
    owners = lax.axis_size("table")
    devices = owners * lax.axis_size("dp")
    table_count, shard_rows, emb_width = tables.shape
    owner_now = owner_ids[0, :, :, 0]
    rows_now = row_ids[0]
    imp_count = owner_now.shape[1]
    capacity = 2 * imp_count // owners
    slot_total = owners * capacity
    one_hot = (owner_now[:, :, None] == jnp.arange(owners, dtype=jnp.int32)).astype(jnp.float32)
    places = jnp.arange(imp_count, dtype=jnp.int32)
    lower_tri = (places[:, None] >= places[None, :]).astype(jnp.float32)
    running = jnp.einsum("ij,tjo->tio", lower_tri, one_hot, precision=lax.Precision.HIGHEST)
    rank_in = (jnp.sum(running * one_hot, axis=2) - 1.0).astype(jnp.int32)
    slot_of = owner_now * capacity + rank_in
    slot_hot = (slot_of[:, :, None] == jnp.arange(slot_total, dtype=jnp.int32)).astype(jnp.int32)
    wanted = jnp.sum(slot_hot * rows_now[:, :, None], axis=1) + shard_rows * (
        1 - jnp.sum(slot_hot, axis=1)
    )
    if (
        capacity % 16 == 0
        and table_count * capacity == 128
        and w_hidden.shape[0] == w_hidden.shape[1]
    ):
        return whole_kernel(
            tables,
            jnp.transpose(wanted.reshape(table_count, owners, capacity), (1, 0, 2)),
            slot_of,
            session_of[0],
            relevance[0],
            logit_bias[0],
            w_hidden,
            bias_hidden,
            w_score,
        )
    requested = lax.all_to_all(
        wanted.reshape(table_count, owners, capacity),
        "table",
        split_axis=1,
        concat_axis=1,
        tiled=True,
    )
    served = lax.map(
        lambda pair: pick_rows(pair[0], pair[1]),
        (requested.reshape(table_count, slot_total), tables),
    )
    served = served.reshape(table_count, owners, capacity, emb_width)
    hidden_bf = w_hidden.astype(jnp.bfloat16)
    returned = lax.all_to_all(served, "table", split_axis=1, concat_axis=1, tiled=True).reshape(
        table_count, slot_total, emb_width
    )
    gathered = lax.map(lambda pair: pick_rows(pair[0], pair[1]), (slot_of, returned))
    inputs = jnp.transpose(gathered, (1, 0, 2)).reshape(imp_count, table_count * emb_width)
    pre_act = jnp.dot(inputs, hidden_bf, preferred_element_type=jnp.float32)
    pre_act = pre_act + bias_hidden
    hidden = jax.nn.silu(pre_act)
    scores = jnp.dot(hidden, w_score, precision=lax.Precision.HIGHEST) + logit_bias[0]
    loss_sum, score_grad = session_terms(scores, session_of[0], relevance[0], SESS_DEV)
    pre_grad = score_grad[:, None] * w_score[None, :] * silu_slope(pre_act)
    pre_grad_bf = pre_grad.astype(jnp.bfloat16)
    weight_grad = lax.dot_general(
        inputs, pre_grad_bf, (((0,), (0,)), ((), ())), preferred_element_type=jnp.float32
    )
    bias_grad = jnp.sum(pre_grad, axis=0)
    score_weight_grad = jnp.dot(score_grad, hidden, precision=lax.Precision.HIGHEST)
    input_grad = jnp.dot(pre_grad_bf, hidden_bf.T, preferred_element_type=jnp.float32).astype(
        jnp.bfloat16
    )
    input_grad = jnp.transpose(input_grad.reshape(imp_count, table_count, emb_width), (1, 0, 2))
    outgoing = lax.map(
        lambda pair: place_rows(pair[0], pair[1], slot_total).astype(jnp.bfloat16),
        (slot_of, input_grad),
    )
    incoming = lax.all_to_all(
        outgoing.reshape(table_count, owners, capacity, emb_width),
        "table",
        split_axis=1,
        concat_axis=1,
        tiled=True,
    )
    summed = lax.map(
        lambda pair: place_rows(pair[0], pair[1], shard_rows),
        (
            requested.reshape(table_count, slot_total),
            incoming.reshape(table_count, slot_total, emb_width),
        ),
    )
    own_rows = lax.psum_scatter(summed, "dp", scatter_dimension=1, tiled=True)
    emb_step = own_rows / (jnp.sqrt(jnp.mean(own_rows * own_rows, axis=2, keepdims=True)) + 1e-06)
    param_count = w_hidden.size + bias_hidden.size + w_score.size
    weight_tot, bias_tot, score_tot, loss_tot = lax.psum(
        (weight_grad, bias_grad, score_weight_grad, loss_sum), ("table", "dp")
    )
    mean_sq = (
        jnp.sum(weight_tot * weight_tot)
        + jnp.sum(bias_tot * bias_tot)
        + jnp.sum(score_tot * score_tot)
    ) / param_count
    factor = 1.0 / jnp.sqrt(mean_sq + 1e-06)
    step_hidden = weight_tot * factor
    loss = loss_tot / (SESS_DEV * devices)
    return (emb_step, step_hidden, bias_tot * factor, score_tot * factor, loss)


MESH = pl.DeviceIdType.MESH


def whole_body(
    sizes, tables_hbm, wanted_ref, slots_ref, columns_ref, weights_ref, bias_ref, scorer_ref,
    emb_ref, step_ref, small_ref,
    tables_ref, ids_in, ids_ref, served, picked, picked_rows, gathered, dense_ref, out_ref,
    load_sem, want_sems, want_own, serve_send, serve_recv, serve_own, grads, swapped, ids_other, emb_rows, from_other, from_plane, from_column, sum_pair, sum_plane,
    total, grad_send, grad_recv, own_sem, swap_send, swap_recv, ids_sems, pair_sems, plane_send,
    plane_recv, column_send, column_recv, emb_sem,
):
    tables, owners, capacity, width, half_rows, inner, outer, hid, sessions, own_sessions = sizes
    slots = owners * capacity
    me = lax.axis_index("table")
    core = lax.axis_index("dp")
    low, high = lax.rem(me, inner), me // inner
    other = (me, 1 - core)

    def load(table):
        return pltpu.make_async_copy(
            tables_hbm.at[table], tables_ref.at[table], load_sem.at[table]
        )

    for table in range(tables):
        load(table).start()
    barrier = pltpu.get_barrier_semaphore()

    def greet(step, carry):
        pl.semaphore_signal(
            barrier, inc=1, device_id=(lax.rem(me + step, owners), core), device_id_type=MESH
        )
        return carry

    pl.semaphore_signal(barrier, inc=1, device_id=other, device_id_type=MESH)
    lax.fori_loop(1, owners, greet, 0)
    pl.semaphore_wait(barrier, owners)

    def remote(src, dst, send, recv, to):
        return pltpu.make_async_remote_copy(
            src_ref=src, dst_ref=dst, send_sem=send, recv_sem=recv, device_id=to,
            device_id_type=MESH,
        )

    def to_peers(copy_to):
        def one(step, carry):
            copy_to(lax.rem(me + step, owners)).start()
            return carry

        lax.fori_loop(1, owners, one, 0)

    to_peers(
        lambda peer: remote(
            wanted_ref.at[peer], ids_in.at[me], want_sems.at[0], want_sems.at[1], (peer, core)
        )
    )
    want_mine = pltpu.make_async_copy(wanted_ref.at[me], ids_in.at[me], want_own.at[0])
    want_mine.start()
    w_bf = weights_ref[...].astype(jnp.bfloat16)
    want_mine.wait()
    remote(
        wanted_ref.at[pl.ds(0, owners - 1)], ids_in.at[pl.ds(0, owners - 1)], want_sems.at[0],
        want_sems.at[1], other,
    ).wait()

    depth = 1024
    shard_rows = 2 * half_rows

    def serve_own_copy(table):
        return pltpu.make_async_copy(
            served.at[table, me], picked.at[table, me], serve_own.at[table]
        )

    for table in range(tables):
        named = jnp.broadcast_to(
            ids_in[:, 0:1, :].astype(jnp.float32), (owners, capacity, 128)
        )
        lane = lax.broadcasted_iota(jnp.int32, named.shape, 2)
        place_in = lax.broadcasted_iota(jnp.int32, named.shape, 1) + table * capacity
        wide_ids = jnp.broadcast_to(
            jnp.sum(jnp.where(lane == place_in, named, 0.0), axis=2, keepdims=True), named.shape
        ).reshape(slots, 128).astype(jnp.int32)
        ids_ref[pl.ds(table, 1), :] = wide_ids.T[0:1, :]
        ids_col = wide_ids[:, 0:1]
        load(table).wait()
        picked_rows[...] = jnp.zeros_like(picked_rows)

        def pick_block(step, carry):
            at = lax.broadcasted_iota(jnp.int32, (slots, depth), 1)
            hot = jnp.where(at == ids_col - step * depth, 1.0, 0.0).astype(jnp.bfloat16)
            rows_at = pl.ds(pl.multiple_of(step * depth, depth), depth)
            picked_rows[...] += jnp.dot(
                hot, tables_ref[table, rows_at, :], preferred_element_type=jnp.float32
            )
            return carry

        lax.fori_loop(0, shard_rows // depth, pick_block, 0)
        served[table] = picked_rows[...].astype(jnp.bfloat16).reshape(owners, capacity, width)
        serve_own_copy(table).start()
        to_peers(
            lambda peer, table=table: remote(
                served.at[table, peer], picked.at[table, me], serve_send.at[table],
                serve_recv.at[table], (peer, core),
            )
        )
    ids_copy = remote(ids_ref, ids_other, ids_sems.at[0], ids_sems.at[1], other)
    ids_copy.start()

    imps = gathered.shape[0]
    for table in range(tables):
        serve_own_copy(table).wait()
        remote(
            served.at[table, pl.ds(0, owners - 1)], picked.at[table, pl.ds(0, owners - 1)],
            serve_send.at[table], serve_recv.at[table], other,
        ).wait()
        slot_col = columns_ref[:, table : table + 1].astype(jnp.int32)
        hot = jnp.where(
            lax.broadcasted_iota(jnp.int32, (imps, slots), 1) == slot_col, 1.0, 0.0
        ).astype(jnp.bfloat16)
        gathered[:, table * width : (table + 1) * width] = jnp.dot(
            hot, picked[table].reshape(slots, width), preferred_element_type=jnp.float32
        ).astype(jnp.bfloat16)
    inputs = gathered[...]
    pre_act = jnp.dot(inputs, w_bf, preferred_element_type=jnp.float32) + bias_ref[...]
    logistic = 1.0 / (1.0 + jnp.exp(-pre_act))
    hidden = pre_act * logistic
    session = columns_ref[:, tables : tables + 1].astype(jnp.int32)
    relevance = columns_ref[:, tables + 1 : tables + 2]
    scores = jnp.sum(hidden * scorer_ref[...], axis=1, keepdims=True)
    scores = scores + columns_ref[:, tables + 2 : tables + 3]
    member = lax.broadcasted_iota(jnp.int32, (imps, 128), 1) == session
    highest = jnp.max(jnp.where(member, scores, -jnp.inf), axis=0, keepdims=True)
    highest_each = jnp.sum(jnp.where(member, highest, 0.0), axis=1, keepdims=True)
    shifted = scores - highest_each
    exponent = jnp.exp(shifted)
    totals = jnp.sum(jnp.where(member, exponent, 0.0), axis=0, keepdims=True)
    weights = jnp.sum(jnp.where(member, relevance, 0.0), axis=0, keepdims=True)
    total_each = jnp.sum(jnp.where(member, totals, 0.0), axis=1, keepdims=True)
    weight_each = jnp.sum(jnp.where(member, weights, 0.0), axis=1, keepdims=True)
    target = relevance / weight_each
    real = lax.broadcasted_iota(jnp.int32, (1, 128), 1) < own_sessions
    loss_sum = jnp.sum(jnp.log(jnp.where(real, totals, 1.0)), keepdims=True) - jnp.sum(
        target * shifted, keepdims=True
    )
    score_grad = exponent / total_each - target
    pre_grad = score_grad * scorer_ref[...] * (logistic * (1.0 + pre_act * (1.0 - logistic)))
    pre_grad_bf = pre_grad.astype(jnp.bfloat16)
    weight_grad = lax.dot_general(
        inputs, pre_grad_bf, (((0,), (0,)), ((), ())), preferred_element_type=jnp.float32
    )
    bias_grad = jnp.sum(pre_grad, axis=0, keepdims=True)
    score_weight_grad = jnp.sum(score_grad * hidden, axis=0, keepdims=True)
    line = lax.broadcasted_iota(jnp.int32, (128, hid), 0)
    spot = lax.broadcasted_iota(jnp.int32, (128, hid), 1)
    extra = jnp.where(line == 0, bias_grad, 0.0) + jnp.where(line == 1, score_weight_grad, 0.0)
    extra = extra + jnp.where((line == 2) & (spot == 0), loss_sum, 0.0)
    dense_ref[:, :, :, :, :hid] = weight_grad.reshape(dense_ref.shape[:4] + (hid,))
    dense_ref[:, :, :, :, hid:] = extra.T.reshape(dense_ref.shape[:4] + (128,))
    pair_up = remote(dense_ref.at[1 - core], from_other, pair_sems.at[0], pair_sems.at[1], other)
    pair_up.start()
    input_grad = lax.dot_general(
        pre_grad_bf, w_bf, (((1,), (1,)), ((), ())), preferred_element_type=jnp.float32
    ).astype(jnp.bfloat16)

    def fill(table):
        hot = jnp.where(
            lax.broadcasted_iota(jnp.int32, (slots, imps), 0) == slots_ref[pl.ds(table, 1), :],
            1.0, 0.0,
        ).astype(jnp.bfloat16)
        out_ref[table] = jnp.dot(
            hot, input_grad[:, table * width : (table + 1) * width],
            preferred_element_type=jnp.float32,
        ).astype(jnp.bfloat16).reshape(owners, capacity, width)

    def own_copy(table):
        return pltpu.make_async_copy(
            out_ref.at[table, me], grads.at[table, me], own_sem.at[table]
        )

    def send_grads(table):
        fill(table)
        own_copy(table).start()

        def send_one(step, carry):
            owner = lax.rem(me + step, owners)
            remote(
                out_ref.at[table, owner], grads.at[table, me], grad_send.at[table],
                grad_recv.at[table], (owner, core),
            ).start()
            return carry

        lax.fori_loop(1, owners, send_one, 0)

    def all_grads(table):
        return remote(
            out_ref.at[table, pl.ds(0, owners - 1)], grads.at[table, pl.ds(0, owners - 1)],
            grad_send.at[table], grad_recv.at[table], other,
        )

    def swap(table):
        return remote(
            grads.at[table], swapped.at[table], swap_send.at[table], swap_recv.at[table], other
        )

    def arrive(table):
        own_copy(table).wait()
        all_grads(table).wait()
        swap(table).start()

    block = 256

    def emb_copy(table):
        return pltpu.make_async_copy(emb_rows.at[table], emb_ref.at[table], emb_sem.at[table])

    def place(table):
        swap(table).wait()
        ids_mine = ids_ref[pl.ds(table, 1), :]
        ids_theirs = ids_other[pl.ds(table, 1), :]
        rows_mine = grads[table].reshape(slots, width)
        rows_theirs = swapped[table].reshape(slots, width)

        def place_block(step, carry):
            at = lax.broadcasted_iota(jnp.int32, (block, slots), 0) + (
                core * half_rows + step * block
            )
            hot_mine = jnp.where(at == ids_mine, 1.0, 0.0).astype(jnp.bfloat16)
            hot_theirs = jnp.where(at == ids_theirs, 1.0, 0.0).astype(jnp.bfloat16)
            summed = jnp.dot(hot_mine, rows_mine, preferred_element_type=jnp.float32)
            summed = summed + jnp.dot(hot_theirs, rows_theirs, preferred_element_type=jnp.float32)
            mean = jnp.sum(summed * summed, axis=1, keepdims=True) / width
            emb_rows[table, pl.ds(pl.multiple_of(step * block, block), block), :] = summed / (
                jnp.sqrt(mean) + 1e-06
            )
            return carry

        lax.fori_loop(0, half_rows // block, place_block, 0)
        emb_copy(table).start()

    def plane_copies(phase, src_of, dst_of):
        return [
            remote(
                src_of(lax.rem(low + step, inner)), dst_of(step - 1), plane_send.at[phase, step - 1],
                plane_recv.at[phase, step - 1], (high * inner + lax.rem(low + step, inner), core),
            )
            for step in range(1, inner)
        ]

    def column_copies(phase, src_of, dst_of):
        return [
            remote(
                src_of(lax.rem(high + step, outer)), dst_of(step - 1), column_send.at[phase, step - 1],
                column_recv.at[phase, step - 1], (lax.rem(high + step, outer) * inner + low, core),
            )
            for step in range(1, outer)
        ]

    def run(copies):
        for copy in copies:
            copy.start()

    def finish(copies):
        for copy in copies:
            copy.wait()

    send_grads(0)
    pair_up.wait()
    sum_pair[...] = dense_ref[core] + from_other[...]
    plane_sum = plane_copies(0, lambda to: sum_pair.at[to], lambda slot: from_plane.at[slot])
    run(plane_sum)
    for table in range(1, tables):
        send_grads(table)
    ids_copy.wait()
    finish(plane_sum)
    part = sum_pair[low]
    for slot in range(inner - 1):
        part = part + from_plane[slot]
    sum_plane[...] = part
    column_sum = column_copies(0, lambda to: sum_plane.at[to], lambda slot: from_column.at[slot])
    run(column_sum)
    arrive(0)
    finish(column_sum)
    part = sum_plane[high]
    for slot in range(outer - 1):
        part = part + from_column[slot]
    total[core, low, high] = part
    column_share = column_copies(
        1, lambda to: total.at[core, low, high], lambda slot: total.at[core, low, high]
    )
    run(column_share)
    place(0)
    for table in range(1, tables):
        if table == 1:
            finish(column_share)
            plane_share = plane_copies(
                1, lambda to: total.at[core, low], lambda slot: total.at[core, low]
            )
            run(plane_share)
        arrive(table)
        if table == tables - 1:
            finish(plane_share)
            pair_down = remote(
                total.at[core], total.at[core], pair_sems.at[2], pair_sems.at[3], other
            )
            pair_down.start()
        place(table)
    pair_down.wait()
    every = total[...].reshape(2 * owners * dense_ref.shape[3], dense_ref.shape[4])
    weights, extra = every[:, :hid], every[:, hid:]
    counted = lax.broadcasted_iota(jnp.int32, extra.shape, 1) < 2
    counts = jnp.where(counted, extra, 0.0)
    squares = jnp.sum(weights * weights, keepdims=True) + jnp.sum(counts * counts, keepdims=True)
    factor = 1.0 / jnp.sqrt(squares / (hid * hid + 2 * hid) + 1e-06)
    step_ref[...] = weights * factor
    scaled = jnp.where(counted, extra * factor, extra / sessions)
    small_ref[...] = scaled.T
    for table in range(tables):
        emb_copy(table).wait()


def whole_kernel(
    tables, wanted, slot_of, session, relevance, logit_bias, w_hidden, bias_hidden, w_score
):
    table_count, shard_rows, width = tables.shape
    owners, _, capacity = wanted.shape
    hid = w_hidden.shape[1]
    imps = session.shape[0]
    slots = owners * capacity
    half_rows = shard_rows // 2
    inner = 1
    while inner * inner < owners:
        inner *= 2
    outer = owners // inner
    rows = hid // (2 * owners)
    wide = hid + 128
    wanted = jnp.broadcast_to(
        wanted.reshape(owners, 1, table_count * capacity), (owners, 8, table_count * capacity)
    )
    columns = jnp.stack(
        [slot_of[table].astype(jnp.float32) for table in range(table_count)]
        + [session.astype(jnp.float32), relevance, logit_bias],
        axis=1,
    )
    sizes = (
        table_count, owners, capacity, width, half_rows, inner, outer, hid,
        SESS_DEV * owners * 2, SESS_DEV,
    )
    f32, bf16 = jnp.float32, jnp.bfloat16
    dma = pltpu.SemaphoreType.DMA
    vmem = pl.BlockSpec(memory_space=pltpu.VMEM)
    emb_step, step_hidden, small = pl.pallas_call(
        functools.partial(whole_body, sizes),
        out_shape=(
            jax.ShapeDtypeStruct((table_count, half_rows, width), f32),
            jax.ShapeDtypeStruct((hid, hid), f32),
            jax.ShapeDtypeStruct((128, hid), f32),
        ),
        in_specs=[pl.BlockSpec(memory_space=pl.ANY)] + [vmem] * 6,
        out_specs=(pl.BlockSpec(memory_space=pl.ANY), vmem, vmem),
        scratch_shapes=[
            pltpu.VMEM(tables.shape, bf16),
            pltpu.VMEM(wanted.shape, jnp.int32),
            pltpu.VMEM((table_count, slots), jnp.int32),
            pltpu.VMEM((table_count, owners, capacity, width), bf16),
            pltpu.VMEM((table_count, owners, capacity, width), bf16),
            pltpu.VMEM((slots, width), f32),
            pltpu.VMEM((imps, table_count * width), bf16),
            pltpu.VMEM((2, inner, outer, rows, wide), f32),
            pltpu.VMEM((table_count, owners, capacity, width), bf16),
            dma((table_count,)), dma((2,)), dma((1,)),
            dma((table_count,)), dma((table_count,)), dma((table_count,)),
            pltpu.VMEM((table_count, owners, capacity, width), bf16),
            pltpu.VMEM((table_count, owners, capacity, width), bf16),
            pltpu.VMEM((table_count, slots), jnp.int32),
            pltpu.VMEM((table_count, half_rows, width), f32),
            pltpu.VMEM((inner, outer, rows, wide), f32),
            pltpu.VMEM((inner - 1, outer, rows, wide), f32),
            pltpu.VMEM((outer - 1, rows, wide), f32),
            pltpu.VMEM((inner, outer, rows, wide), f32),
            pltpu.VMEM((outer, rows, wide), f32),
            pltpu.VMEM((2, inner, outer, rows, wide), f32),
            dma((table_count,)), dma((table_count,)), dma((table_count,)),
            dma((table_count,)), dma((table_count,)),
            dma((2,)), dma((4,)),
            dma((2, inner - 1)), dma((2, inner - 1)), dma((2, outer - 1)), dma((2, outer - 1)),
            dma((table_count,)),
        ],
        compiler_params=pltpu.CompilerParams(
            collective_id=1, has_side_effects=True, vmem_limit_bytes=60 * 1024 * 1024
        ),
    )(tables, wanted, slot_of, columns, w_hidden, bias_hidden[None, :], w_score[None, :])
    return (emb_step, step_hidden, small[0], small[1], small[2, 0])


def solution(mesh):
    in_specs = (
        P(None, "table", None),
        P(("table", "dp"), None, None, None),
        P(("table", "dp"), None, None),
        P(("table", "dp"), None),
        P(("table", "dp"), None),
        P(("table", "dp"), None),
        P(),
        P(),
        P(),
    )
    out_specs = (P(None, ("table", "dp"), None), P(), P(), P(), P())
    return jax.shard_map(
        on_device, mesh=mesh, in_specs=in_specs, out_specs=out_specs, check_vma=False
    )
```

```python
import jax
import jax.numpy as jnp
from jax import lax
from jax.experimental import pallas as pl
from jax.experimental.pallas import tpu as pltpu
import functools
from jax.sharding import PartitionSpec as P

SESS_DEV = 2


def silu_slope(pre_val):
    logistic = jax.nn.sigmoid(pre_val)
    return logistic * (1.0 + pre_val * (1.0 - logistic))


def session_terms(scores, session_ids, relevance, sessions):
    member = session_ids[None, :] == jnp.arange(sessions, dtype=jnp.int32)[:, None]
    highest = jnp.max(jnp.where(member, scores[None, :], -jnp.inf), axis=1)
    highest_each = jnp.sum(jnp.where(member, highest[:, None], 0.0), axis=0)
    shifted = scores - highest_each
    exponent = jnp.exp(shifted)
    totals = jnp.sum(jnp.where(member, exponent[None, :], 0.0), axis=1)
    weights = jnp.sum(jnp.where(member, relevance[None, :], 0.0), axis=1)
    total_each = jnp.sum(jnp.where(member, totals[:, None], 0.0), axis=0)
    weight_each = jnp.sum(jnp.where(member, weights[:, None], 0.0), axis=0)
    probability = exponent / total_each
    target = relevance / weight_each
    loss_sum = jnp.sum(jnp.log(totals)) - jnp.sum(target * shifted)
    return (loss_sum, probability - target)


def selector(indices, count):
    return (indices[:, None] == jnp.arange(count, dtype=jnp.int32)[None, :]).astype(jnp.bfloat16)


def pick_rows(indices, source):
    return jnp.dot(
        selector(indices, source.shape[0]), source, preferred_element_type=jnp.float32
    ).astype(jnp.bfloat16)


def place_rows(indices, values, count):
    return lax.dot_general(
        selector(indices, count),
        values,
        (((0,), (0,)), ((), ())),
        preferred_element_type=jnp.float32,
    )


def on_device(
    tables, owner_ids, row_ids, session_of, relevance, logit_bias, w_hidden, bias_hidden, w_score
):
    owners = lax.axis_size("table")
    devices = owners * lax.axis_size("dp")
    table_count, shard_rows, emb_width = tables.shape
    owner_now = owner_ids[0, :, :, 0]
    rows_now = row_ids[0]
    imp_count = owner_now.shape[1]
    capacity = 2 * imp_count // owners
    slot_total = owners * capacity
    one_hot = (owner_now[:, :, None] == jnp.arange(owners, dtype=jnp.int32)).astype(jnp.float32)
    places = jnp.arange(imp_count, dtype=jnp.int32)
    lower_tri = (places[:, None] >= places[None, :]).astype(jnp.float32)
    running = jnp.einsum("ij,tjo->tio", lower_tri, one_hot, precision=lax.Precision.HIGHEST)
    rank_in = (jnp.sum(running * one_hot, axis=2) - 1.0).astype(jnp.int32)
    slot_of = owner_now * capacity + rank_in
    slot_hot = (slot_of[:, :, None] == jnp.arange(slot_total, dtype=jnp.int32)).astype(jnp.int32)
    wanted = jnp.sum(slot_hot * rows_now[:, :, None], axis=1) + shard_rows * (
        1 - jnp.sum(slot_hot, axis=1)
    )
    if (
        capacity % 16 == 0
        and table_count * capacity == 128
        and w_hidden.shape[0] == w_hidden.shape[1]
    ):
        return whole_kernel(
            tables,
            jnp.transpose(wanted.reshape(table_count, owners, capacity), (1, 0, 2)),
            slot_of,
            session_of[0],
            relevance[0],
            logit_bias[0],
            w_hidden,
            bias_hidden,
            w_score,
        )
    requested = lax.all_to_all(
        wanted.reshape(table_count, owners, capacity),
        "table",
        split_axis=1,
        concat_axis=1,
        tiled=True,
    )
    served = lax.map(
        lambda pair: pick_rows(pair[0], pair[1]),
        (requested.reshape(table_count, slot_total), tables),
    )
    served = served.reshape(table_count, owners, capacity, emb_width)
    hidden_bf = w_hidden.astype(jnp.bfloat16)
    returned = lax.all_to_all(served, "table", split_axis=1, concat_axis=1, tiled=True).reshape(
        table_count, slot_total, emb_width
    )
    gathered = lax.map(lambda pair: pick_rows(pair[0], pair[1]), (slot_of, returned))
    inputs = jnp.transpose(gathered, (1, 0, 2)).reshape(imp_count, table_count * emb_width)
    pre_act = jnp.dot(inputs, hidden_bf, preferred_element_type=jnp.float32)
    pre_act = pre_act + bias_hidden
    hidden = jax.nn.silu(pre_act)
    scores = jnp.dot(hidden, w_score, precision=lax.Precision.HIGHEST) + logit_bias[0]
    loss_sum, score_grad = session_terms(scores, session_of[0], relevance[0], SESS_DEV)
    pre_grad = score_grad[:, None] * w_score[None, :] * silu_slope(pre_act)
    pre_grad_bf = pre_grad.astype(jnp.bfloat16)
    weight_grad = lax.dot_general(
        inputs, pre_grad_bf, (((0,), (0,)), ((), ())), preferred_element_type=jnp.float32
    )
    bias_grad = jnp.sum(pre_grad, axis=0)
    score_weight_grad = jnp.dot(score_grad, hidden, precision=lax.Precision.HIGHEST)
    input_grad = jnp.dot(pre_grad_bf, hidden_bf.T, preferred_element_type=jnp.float32).astype(
        jnp.bfloat16
    )
    input_grad = jnp.transpose(input_grad.reshape(imp_count, table_count, emb_width), (1, 0, 2))
    outgoing = lax.map(
        lambda pair: place_rows(pair[0], pair[1], slot_total).astype(jnp.bfloat16),
        (slot_of, input_grad),
    )
    incoming = lax.all_to_all(
        outgoing.reshape(table_count, owners, capacity, emb_width),
        "table",
        split_axis=1,
        concat_axis=1,
        tiled=True,
    )
    summed = lax.map(
        lambda pair: place_rows(pair[0], pair[1], shard_rows),
        (
            requested.reshape(table_count, slot_total),
            incoming.reshape(table_count, slot_total, emb_width),
        ),
    )
    own_rows = lax.psum_scatter(summed, "dp", scatter_dimension=1, tiled=True)
    emb_step = own_rows / (jnp.sqrt(jnp.mean(own_rows * own_rows, axis=2, keepdims=True)) + 1e-06)
    param_count = w_hidden.size + bias_hidden.size + w_score.size
    weight_tot, bias_tot, score_tot, loss_tot = lax.psum(
        (weight_grad, bias_grad, score_weight_grad, loss_sum), ("table", "dp")
    )
    mean_sq = (
        jnp.sum(weight_tot * weight_tot)
        + jnp.sum(bias_tot * bias_tot)
        + jnp.sum(score_tot * score_tot)
    ) / param_count
    factor = 1.0 / jnp.sqrt(mean_sq + 1e-06)
    step_hidden = weight_tot * factor
    loss = loss_tot / (SESS_DEV * devices)
    return (emb_step, step_hidden, bias_tot * factor, score_tot * factor, loss)


MESH = pl.DeviceIdType.MESH


def whole_body(
    sizes, tables_hbm, wanted_ref, slots_ref, columns_ref, weights_ref, bias_ref, scorer_ref,
    emb_ref, step_ref, small_ref,
    tables_ref, ids_in, ids_ref, served, picked, picked_rows, gathered, dense_ref, out_ref,
    load_sem, want_sems, want_own, serve_send, serve_recv, serve_own, grads, swapped, ids_other, emb_rows, from_other, from_plane, from_column, sum_pair, sum_plane,
    total, grad_send, grad_recv, own_sem, swap_send, swap_recv, ids_sems, pair_sems, plane_send,
    plane_recv, column_send, column_recv, emb_sem,
):
    tables, owners, capacity, width, half_rows, inner, outer, hid, sessions, own_sessions = sizes
    slots = owners * capacity
    me = lax.axis_index("table")
    core = lax.axis_index("dp")
    low, high = lax.rem(me, inner), me // inner
    other = (me, 1 - core)

    def load(table):
        return pltpu.make_async_copy(
            tables_hbm.at[table], tables_ref.at[table], load_sem.at[table]
        )

    for table in range(tables):
        load(table).start()
    barrier = pltpu.get_barrier_semaphore()

    def greet(step, carry):
        pl.semaphore_signal(
            barrier, inc=1, device_id=(lax.rem(me + step, owners), core), device_id_type=MESH
        )
        return carry

    pl.semaphore_signal(barrier, inc=1, device_id=other, device_id_type=MESH)
    lax.fori_loop(1, owners, greet, 0)
    pl.semaphore_wait(barrier, owners)

    def remote(src, dst, send, recv, to):
        return pltpu.make_async_remote_copy(
            src_ref=src, dst_ref=dst, send_sem=send, recv_sem=recv, device_id=to,
            device_id_type=MESH,
        )

    def to_peers(copy_to):
        def one(step, carry):
            copy_to(lax.rem(me + step, owners)).start()
            return carry

        lax.fori_loop(1, owners, one, 0)

    to_peers(
        lambda peer: remote(
            wanted_ref.at[peer], ids_in.at[me], want_sems.at[0], want_sems.at[1], (peer, core)
        )
    )
    want_mine = pltpu.make_async_copy(wanted_ref.at[me], ids_in.at[me], want_own.at[0])
    want_mine.start()
    w_bf = weights_ref[...].astype(jnp.bfloat16)
    want_mine.wait()
    remote(
        wanted_ref.at[pl.ds(0, owners - 1)], ids_in.at[pl.ds(0, owners - 1)], want_sems.at[0],
        want_sems.at[1], other,
    ).wait()

    depth = 1024
    shard_rows = 2 * half_rows

    def serve_own_copy(table):
        return pltpu.make_async_copy(
            served.at[table, me], picked.at[table, me], serve_own.at[table]
        )

    for table in range(tables):
        named = jnp.broadcast_to(
            ids_in[:, 0:1, :].astype(jnp.float32), (owners, capacity, 128)
        )
        lane = lax.broadcasted_iota(jnp.int32, named.shape, 2)
        place_in = lax.broadcasted_iota(jnp.int32, named.shape, 1) + table * capacity
        wide_ids = jnp.broadcast_to(
            jnp.sum(jnp.where(lane == place_in, named, 0.0), axis=2, keepdims=True), named.shape
        ).reshape(slots, 128).astype(jnp.int32)
        ids_ref[pl.ds(table, 1), :] = wide_ids.T[0:1, :]
        ids_col = wide_ids[:, 0:1]
        load(table).wait()
        picked_rows[...] = jnp.zeros_like(picked_rows)

        def pick_block(step, carry):
            at = lax.broadcasted_iota(jnp.int32, (slots, depth), 1)
            hot = jnp.where(at == ids_col - step * depth, 1.0, 0.0).astype(jnp.bfloat16)
            rows_at = pl.ds(pl.multiple_of(step * depth, depth), depth)
            picked_rows[...] += jnp.dot(
                hot, tables_ref[table, rows_at, :], preferred_element_type=jnp.float32
            )
            return carry

        lax.fori_loop(0, shard_rows // depth, pick_block, 0)
        served[table] = picked_rows[...].astype(jnp.bfloat16).reshape(owners, capacity, width)
        serve_own_copy(table).start()
        to_peers(
            lambda peer, table=table: remote(
                served.at[table, peer], picked.at[table, me], serve_send.at[table],
                serve_recv.at[table], (peer, core),
            )
        )
    ids_copy = remote(ids_ref, ids_other, ids_sems.at[0], ids_sems.at[1], other)
    ids_copy.start()

    imps = gathered.shape[0]
    for table in range(tables):
        serve_own_copy(table).wait()
        remote(
            served.at[table, pl.ds(0, owners - 1)], picked.at[table, pl.ds(0, owners - 1)],
            serve_send.at[table], serve_recv.at[table], other,
        ).wait()
        slot_col = columns_ref[:, table : table + 1].astype(jnp.int32)
        hot = jnp.where(
            lax.broadcasted_iota(jnp.int32, (imps, slots), 1) == slot_col, 1.0, 0.0
        ).astype(jnp.bfloat16)
        gathered[:, table * width : (table + 1) * width] = jnp.dot(
            hot, picked[table].reshape(slots, width), preferred_element_type=jnp.float32
        ).astype(jnp.bfloat16)
    inputs = gathered[...]
    pre_act = jnp.dot(inputs, w_bf, preferred_element_type=jnp.float32) + bias_ref[...]
    logistic = 1.0 / (1.0 + jnp.exp(-pre_act))
    hidden = pre_act * logistic
    session = columns_ref[:, tables : tables + 1].astype(jnp.int32)
    relevance = columns_ref[:, tables + 1 : tables + 2]
    scores = jnp.sum(hidden * scorer_ref[...], axis=1, keepdims=True)
    scores = scores + columns_ref[:, tables + 2 : tables + 3]
    member = lax.broadcasted_iota(jnp.int32, (imps, 128), 1) == session
    highest = jnp.max(jnp.where(member, scores, -jnp.inf), axis=0, keepdims=True)
    highest_each = jnp.sum(jnp.where(member, highest, 0.0), axis=1, keepdims=True)
    shifted = scores - highest_each
    exponent = jnp.exp(shifted)
    totals = jnp.sum(jnp.where(member, exponent, 0.0), axis=0, keepdims=True)
    weights = jnp.sum(jnp.where(member, relevance, 0.0), axis=0, keepdims=True)
    total_each = jnp.sum(jnp.where(member, totals, 0.0), axis=1, keepdims=True)
    weight_each = jnp.sum(jnp.where(member, weights, 0.0), axis=1, keepdims=True)
    target = relevance / weight_each
    real = lax.broadcasted_iota(jnp.int32, (1, 128), 1) < own_sessions
    loss_sum = jnp.sum(jnp.log(jnp.where(real, totals, 1.0)), keepdims=True) - jnp.sum(
        target * shifted, keepdims=True
    )
    score_grad = exponent / total_each - target
    pre_grad = score_grad * scorer_ref[...] * (logistic * (1.0 + pre_act * (1.0 - logistic)))
    pre_grad_bf = pre_grad.astype(jnp.bfloat16)
    weight_grad = lax.dot_general(
        inputs, pre_grad_bf, (((0,), (0,)), ((), ())), preferred_element_type=jnp.float32
    )
    bias_grad = jnp.sum(pre_grad, axis=0, keepdims=True)
    score_weight_grad = jnp.sum(score_grad * hidden, axis=0, keepdims=True)
    line = lax.broadcasted_iota(jnp.int32, (128, hid), 0)
    spot = lax.broadcasted_iota(jnp.int32, (128, hid), 1)
    extra = jnp.where(line == 0, bias_grad, 0.0) + jnp.where(line == 1, score_weight_grad, 0.0)
    extra = extra + jnp.where((line == 2) & (spot == 0), loss_sum, 0.0)
    dense_ref[:, :, :, :, :hid] = weight_grad.reshape(dense_ref.shape[:4] + (hid,))
    dense_ref[:, :, :, :, hid:] = extra.T.reshape(dense_ref.shape[:4] + (128,))
    pair_up = remote(dense_ref.at[1 - core], from_other, pair_sems.at[0], pair_sems.at[1], other)
    pair_up.start()
    input_grad = lax.dot_general(
        pre_grad_bf, w_bf, (((1,), (1,)), ((), ())), preferred_element_type=jnp.float32
    ).astype(jnp.bfloat16)

    def fill(table):
        hot = jnp.where(
            lax.broadcasted_iota(jnp.int32, (slots, imps), 0) == slots_ref[pl.ds(table, 1), :],
            1.0, 0.0,
        ).astype(jnp.bfloat16)
        out_ref[table] = jnp.dot(
            hot, input_grad[:, table * width : (table + 1) * width],
            preferred_element_type=jnp.float32,
        ).astype(jnp.bfloat16).reshape(owners, capacity, width)

    def own_copy(table):
        return pltpu.make_async_copy(
            out_ref.at[table, me], grads.at[table, me], own_sem.at[table]
        )

    def send_grads(table):
        fill(table)
        own_copy(table).start()

        def send_one(step, carry):
            owner = lax.rem(me + step, owners)
            remote(
                out_ref.at[table, owner], grads.at[table, me], grad_send.at[table],
                grad_recv.at[table], (owner, core),
            ).start()
            return carry

        lax.fori_loop(1, owners, send_one, 0)

    def all_grads(table):
        return remote(
            out_ref.at[table, pl.ds(0, owners - 1)], grads.at[table, pl.ds(0, owners - 1)],
            grad_send.at[table], grad_recv.at[table], other,
        )

    def swap(table):
        return remote(
            grads.at[table], swapped.at[table], swap_send.at[table], swap_recv.at[table], other
        )

    def arrive(table):
        own_copy(table).wait()
        all_grads(table).wait()
        swap(table).start()

    block = 256

    def emb_copy(table):
        return pltpu.make_async_copy(emb_rows.at[table], emb_ref.at[table], emb_sem.at[table])

    def place(table):
        swap(table).wait()
        ids_mine = ids_ref[pl.ds(table, 1), :]
        ids_theirs = ids_other[pl.ds(table, 1), :]
        rows_mine = grads[table].reshape(slots, width)
        rows_theirs = swapped[table].reshape(slots, width)

        def place_block(step, carry):
            at = lax.broadcasted_iota(jnp.int32, (block, slots), 0) + (
                core * half_rows + step * block
            )
            hot_mine = jnp.where(at == ids_mine, 1.0, 0.0).astype(jnp.bfloat16)
            hot_theirs = jnp.where(at == ids_theirs, 1.0, 0.0).astype(jnp.bfloat16)
            summed = jnp.dot(hot_mine, rows_mine, preferred_element_type=jnp.float32)
            summed = summed + jnp.dot(hot_theirs, rows_theirs, preferred_element_type=jnp.float32)
            mean = jnp.sum(summed * summed, axis=1, keepdims=True) / width
            emb_rows[table, pl.ds(pl.multiple_of(step * block, block), block), :] = summed / (
                jnp.sqrt(mean) + 1e-06
            )
            return carry

        lax.fori_loop(0, half_rows // block, place_block, 0)
        emb_copy(table).start()

    def plane_copies(phase, src_of, dst_of):
        return [
            remote(
                src_of(lax.rem(low + step, inner)), dst_of(step - 1), plane_send.at[phase, step - 1],
                plane_recv.at[phase, step - 1], (high * inner + lax.rem(low + step, inner), core),
            )
            for step in range(1, inner)
        ]

    def column_copies(phase, src_of, dst_of):
        return [
            remote(
                src_of(lax.rem(high + step, outer)), dst_of(step - 1), column_send.at[phase, step - 1],
                column_recv.at[phase, step - 1], (lax.rem(high + step, outer) * inner + low, core),
            )
            for step in range(1, outer)
        ]

    def run(copies):
        for copy in copies:
            copy.start()

    def finish(copies):
        for copy in copies:
            copy.wait()

    send_grads(0)
    pair_up.wait()
    sum_pair[...] = dense_ref[core] + from_other[...]
    plane_sum = plane_copies(0, lambda to: sum_pair.at[to], lambda slot: from_plane.at[slot])
    run(plane_sum)
    send_grads(1)
    ids_copy.wait()
    finish(plane_sum)
    part = sum_pair[low]
    for slot in range(inner - 1):
        part = part + from_plane[slot]
    sum_plane[...] = part
    column_sum = column_copies(0, lambda to: sum_plane.at[to], lambda slot: from_column.at[slot])
    run(column_sum)
    send_grads(2)
    arrive(0)
    finish(column_sum)
    part = sum_plane[high]
    for slot in range(outer - 1):
        part = part + from_column[slot]
    total[core, low, high] = part
    column_share = column_copies(
        1, lambda to: total.at[core, low, high], lambda slot: total.at[core, low, high]
    )
    run(column_share)

    def plane_share(step):
        source = lax.rem(high + outer - step, outer)
        return plane_copies(
            1 + step,
            lambda to: total.at[core, low, source],
            lambda slot: total.at[core, low, source],
        )

    run(plane_share(0))
    for table in range(3, tables):
        send_grads(table)
    place(0)
    for step in range(1, outer):
        column_share[step - 1].wait()
        run(plane_share(step))
    for table in range(1, tables):
        arrive(table)
        if table == tables - 1:
            for step in range(outer):
                finish(plane_share(step))
            pair_down = remote(
                total.at[core], total.at[core], pair_sems.at[2], pair_sems.at[3], other
            )
            pair_down.start()
        place(table)
    pair_down.wait()
    every = total[...].reshape(2 * owners * dense_ref.shape[3], dense_ref.shape[4])
    weights, extra = every[:, :hid], every[:, hid:]
    counted = lax.broadcasted_iota(jnp.int32, extra.shape, 1) < 2
    counts = jnp.where(counted, extra, 0.0)
    squares = jnp.sum(weights * weights, keepdims=True) + jnp.sum(counts * counts, keepdims=True)
    factor = 1.0 / jnp.sqrt(squares / (hid * hid + 2 * hid) + 1e-06)
    step_ref[...] = weights * factor
    scaled = jnp.where(counted, extra * factor, extra / sessions)
    small_ref[...] = scaled.T
    for table in range(tables):
        emb_copy(table).wait()


def whole_kernel(
    tables, wanted, slot_of, session, relevance, logit_bias, w_hidden, bias_hidden, w_score
):
    table_count, shard_rows, width = tables.shape
    owners, _, capacity = wanted.shape
    hid = w_hidden.shape[1]
    imps = session.shape[0]
    slots = owners * capacity
    half_rows = shard_rows // 2
    inner = 1
    while inner * inner < owners:
        inner *= 2
    outer = owners // inner
    rows = hid // (2 * owners)
    wide = hid + 128
    wanted = jnp.broadcast_to(
        wanted.reshape(owners, 1, table_count * capacity), (owners, 8, table_count * capacity)
    )
    columns = jnp.stack(
        [slot_of[table].astype(jnp.float32) for table in range(table_count)]
        + [session.astype(jnp.float32), relevance, logit_bias],
        axis=1,
    )
    sizes = (
        table_count, owners, capacity, width, half_rows, inner, outer, hid,
        SESS_DEV * owners * 2, SESS_DEV,
    )
    f32, bf16 = jnp.float32, jnp.bfloat16
    dma = pltpu.SemaphoreType.DMA
    vmem = pl.BlockSpec(memory_space=pltpu.VMEM)
    emb_step, step_hidden, small = pl.pallas_call(
        functools.partial(whole_body, sizes),
        out_shape=(
            jax.ShapeDtypeStruct((table_count, half_rows, width), f32),
            jax.ShapeDtypeStruct((hid, hid), f32),
            jax.ShapeDtypeStruct((128, hid), f32),
        ),
        in_specs=[pl.BlockSpec(memory_space=pl.ANY)] + [vmem] * 6,
        out_specs=(pl.BlockSpec(memory_space=pl.ANY), vmem, vmem),
        scratch_shapes=[
            pltpu.VMEM(tables.shape, bf16),
            pltpu.VMEM(wanted.shape, jnp.int32),
            pltpu.VMEM((table_count, slots), jnp.int32),
            pltpu.VMEM((table_count, owners, capacity, width), bf16),
            pltpu.VMEM((table_count, owners, capacity, width), bf16),
            pltpu.VMEM((slots, width), f32),
            pltpu.VMEM((imps, table_count * width), bf16),
            pltpu.VMEM((2, inner, outer, rows, wide), f32),
            pltpu.VMEM((table_count, owners, capacity, width), bf16),
            dma((table_count,)), dma((2,)), dma((1,)),
            dma((table_count,)), dma((table_count,)), dma((table_count,)),
            pltpu.VMEM((table_count, owners, capacity, width), bf16),
            pltpu.VMEM((table_count, owners, capacity, width), bf16),
            pltpu.VMEM((table_count, slots), jnp.int32),
            pltpu.VMEM((table_count, half_rows, width), f32),
            pltpu.VMEM((inner, outer, rows, wide), f32),
            pltpu.VMEM((inner - 1, outer, rows, wide), f32),
            pltpu.VMEM((outer - 1, rows, wide), f32),
            pltpu.VMEM((inner, outer, rows, wide), f32),
            pltpu.VMEM((outer, rows, wide), f32),
            pltpu.VMEM((2, inner, outer, rows, wide), f32),
            dma((table_count,)), dma((table_count,)), dma((table_count,)),
            dma((table_count,)), dma((table_count,)),
            dma((2,)), dma((4,)),
            dma((1 + outer, inner - 1)), dma((1 + outer, inner - 1)), dma((2, outer - 1)), dma((2, outer - 1)),
            dma((table_count,)),
        ],
        compiler_params=pltpu.CompilerParams(
            collective_id=1, has_side_effects=True, vmem_limit_bytes=60 * 1024 * 1024
        ),
    )(tables, wanted, slot_of, columns, w_hidden, bias_hidden[None, :], w_score[None, :])
    return (emb_step, step_hidden, small[0], small[1], small[2, 0])


def solution(mesh):
    in_specs = (
        P(None, "table", None),
        P(("table", "dp"), None, None, None),
        P(("table", "dp"), None, None),
        P(("table", "dp"), None),
        P(("table", "dp"), None),
        P(("table", "dp"), None),
        P(),
        P(),
        P(),
    )
    out_specs = (P(None, ("table", "dp"), None), P(), P(), P(), P())
    return jax.shard_map(
        on_device, mesh=mesh, in_specs=in_specs, out_specs=out_specs, check_vma=False
    )
```
